32 devices in a mesh: row: 8 (over y, x, core), col: 4 (over z).
Axes of the slice: x: 2, y: 2, z: 4, core: 2. Of those that a mesh axis runs over, the one named last changes fastest.
Arguments:
- surface: bfloat16 [16384, 16384], P('row', 'col'), may hold values from -0.0234375 to 0.0234375
- excitation: float32 [16384, 128], P(('row', 'col')), may hold values from -6 to 6
- dtn_blocks: bfloat16 [32, 1024, 1024], P(('row', 'col')), may hold values from -0.09375 to 0.09375
- interp_blocks: bfloat16 [32, 1024, 2048], P(('row', 'col')), may hold values from -0.09375 to 0.09375
- adjacency: int32 [32, 6], P(('row', 'col')), may hold values from 0 to 31, as said below
Outputs:
- solution: float32 [16384, 128], P(('row', 'col'))
- residual: float32 [16384, 128], P(('row', 'col'))
The draws below stay inside these ranges and needn't reach their ends.
Inputs may be any that keep to these rules, and one draw needn't show every extreme that they name: `adjacency`: entry [s, k] names a subdomain of the same spatial group as s (equal index // 4); it may name s itself, which adds nothing.
All inputs are finite; a program needn't handle non-finite values.
Results may differ from the reference program's by a relative error of at most 0.02.
Values may be sent and summed in bfloat16 or wider, within the bound.
A program may use at most 64 MiB of HBM per device.

```python
import jax
import jax.numpy as jnp
from jax import lax

NS = 16384
M = 1024
NE = 128
ITERS = 2
NADJ = 6
NSUB = 32
GROUP = 4
RB = 2048
N_ROW = 8


def draw_adjacency(key, part):
    base = jnp.arange(NSUB, dtype=jnp.int32) // GROUP * GROUP
    offsets = jax.random.randint(jax.random.fold_in(key, 17), (NSUB, NADJ), 0, GROUP, dtype=jnp.int32)
    return base[:, None] + offsets


def block_scale(stream_key, shape, cuts, smallest, top_value):
    factor_of = 1.0
    for axis_at, shards_of in cuts:
        steps = jax.random.uniform(jax.random.fold_in(jax.random.fold_in(stream_key, 6), axis_at), (shards_of,), jnp.float32, smallest / len(cuts), top_value / len(cuts))
        factor_of = factor_of * jnp.repeat(jnp.exp(steps), shape[axis_at] // shards_of).reshape((-1,) + (1,) * (len(shape) - 1 - axis_at))
    return factor_of


def gaussian(stream_key, shape, deviation, reach, shards=(), held_as=jnp.bfloat16):
    result = deviation * jax.random.normal(stream_key, shape, jnp.float32)
    if shards:
        result = result * block_scale(stream_key, shape, shards, -0.22, 0.18)
    return jnp.clip(result, -reach, reach).astype(held_as)


def setup_inputs(seed: int = 0) -> dict:
    seeds = jax.random.split(jax.random.key(seed), 6)
    return {
        "surface": gaussian(seeds[0], (NS, NS), (4 * NS) ** -0.5, 0.0234375, ((0, 8), (1, 4))),
        "excitation": gaussian(seeds[1], (NS, NE), 1.0, 6.0, ((0, 32),), jnp.float32),
        "dtn_blocks": gaussian(seeds[2], (NSUB, M, M), (4 * M) ** -0.5, 0.09375, ((0, 32),)),
        "interp_blocks": gaussian(seeds[3], (NSUB, M, RB), (2 * RB) ** -0.5, 0.09375, ((0, 32),)),
        "adjacency": draw_adjacency(jax.random.fold_in(seeds[5], 71), 0),
    }


damping = 0.25
face_weight = 0.25


def reference(surface, excitation, dtn_blocks, interp_blocks, adjacency):
    current = excitation
    residual = excitation
    indices = jnp.arange(NSUB, dtype=jnp.int32)
    for sweep in range(ITERS):
        rounded = current.astype(jnp.bfloat16)
        applied = jnp.dot(surface, rounded, preferred_element_type=jnp.float32)
        grouped = rounded.reshape(N_ROW, RB, NE)

        def trace_one(index):
            block = lax.dynamic_index_in_dim(grouped, index // GROUP, 0, keepdims=False)
            return jnp.dot(interp_blocks[index], block, preferred_element_type=jnp.float32).astype(jnp.bfloat16)

        traces = lax.map(trace_one, indices)

        def respond(index):
            own = traces[index]
            own_wide = own.astype(jnp.float32)
            neighbours = jnp.zeros((M, NE), jnp.float32)
            for slot in range(NADJ):
                neighbours = neighbours + traces[adjacency[index, slot]].astype(jnp.float32)
            combined = jnp.dot(dtn_blocks[index], own, preferred_element_type=jnp.float32) + own_wide
            combined = combined + face_weight * (NADJ * own_wide - neighbours)
            response = combined.astype(jnp.bfloat16)
            return lax.dot_general(interp_blocks[index], response, (((0,), (0,)), ((), ())), preferred_element_type=jnp.float32)

        returned = lax.map(respond, indices)
        back = returned.reshape(N_ROW, GROUP, RB, NE).sum(axis=1).reshape(NS, NE)
        residual = excitation - current - applied - back
        current = current + damping * residual
    return current, residual
```

```python
import functools

import jax
import jax.numpy as jnp
from jax import lax
from jax.experimental import pallas as pl
from jax.experimental.pallas import tpu as pltpu
from jax.sharding import PartitionSpec as P

ITERS = 2
NADJ = 6

damping = 0.25
face_weight = 0.25
F32, BF16 = jnp.float32, jnp.bfloat16


def xor(a, b, bits):
    total = 0
    for i in range(bits):
        x, y = a // 2**i % 2, b // 2**i % 2
        total = total + (x + y - 2 * x * y) * 2**i
    return total


def gray(p, bits):
    return xor(p, p // 2, bits)


def ungray(g, bits):
    total, above = 0, 0
    for i in reversed(range(bits)):
        bit = g // 2**i % 2
        above = above + bit - 2 * above * bit
        total = total + above * 2**i
    return total


def kernel(
    R, n, tile,
    exc_hbm, interp_hbm, surf_hbm, dtn_hbm, adj,
    sol_ref, res_ref,
    exc, interp, surf, dtn, grp, colb, trc, acc, part, sbuf, rbuf,
    load_sem, g_ss, g_rs, t_ss, t_rs, c_ss, c_rs, p_ss, p_rs, r_ss, r_rs,
):
    half_n = n // 2
    bits = n.bit_length() - 1
    _, _, hs, ne = grp.shape[1:]
    m = interp.shape[0]
    rb = interp.shape[1]
    tiles = surf.shape[0] // tile
    r, c = lax.axis_index("row"), lax.axis_index("col")
    core, chip = r % 2, r // 2
    pos = ungray(xor(chip, c, bits), bits)
    right, left = (r, (c + 1) % n), (r, (c + n - 1) % n)
    partner = (chip * 2 + 1 - core, c)
    gnext = (xor(gray((pos + 1) % n, bits), c, bits) * 2 + core, c)
    gprev = (xor(gray((pos + n - 1) % n, bits), c, bits) * 2 + core, c)

    loads = [
        pltpu.make_async_copy(exc_hbm, exc, load_sem.at[0]),
        pltpu.make_async_copy(interp_hbm, interp, load_sem.at[1]),
    ]
    for i in range(tiles):
        rows = pl.ds(i * tile, tile)
        loads.append(pltpu.make_async_copy(surf_hbm.at[rows], surf.at[rows], load_sem.at[3 + i]))
    loads.append(pltpu.make_async_copy(dtn_hbm, dtn, load_sem.at[2]))
    for load in loads:
        load.start()

    barrier = pltpu.get_barrier_semaphore()
    for device in (left, right, partner, gnext, gprev):
        pl.semaphore_signal(barrier, inc=1, device_id=device, device_id_type=pl.DeviceIdType.MESH)
    pl.semaphore_wait(barrier, 5)

    def remote(src, dst, ss, rs, device):
        return pltpu.make_async_remote_copy(
            src_ref=src, dst_ref=dst, send_sem=ss, recv_sem=rs,
            device_id=device, device_id_type=pl.DeviceIdType.MESH,
        )

    def ring(buf, ss, rs, s, d, t, h, receive=False):
        hop = t if receive else t - 1
        owner = (c + n - hop) % n if d == 0 else (c + hop) % n
        block = buf.at[s, owner, h]
        return remote(block, block, ss.at[s, d, t - 1, h], rs.at[s, d, t - 1, h], right if d == 0 else left)

    def halves(d, t):
        if t == half_n:
            return (d,)
        return (d, 1 - d)

    waits = []

    def chain(s, owner, delta):
        def copies(src):
            out = []
            for h in range(2):
                block = src.at[owner, h]
                dst = colb.at[s, core, owner, h]
                k = (s, delta, h)
                out.append((
                    remote(block, dst, c_ss.at[k], c_rs.at[k], gnext if h == 0 else gprev),
                    remote(block, dst, p_ss.at[k], p_rs.at[k], partner),
                ))
            return out

        more = (pos != n - 1, pos != 1)

        @pl.when(pos == 0)
        def _():
            for h, (on, share) in enumerate(copies(grp.at[s])):
                on.start()
                share.start()

        @pl.when(pos != 0)
        def _():
            for h, (on, share) in enumerate(copies(colb.at[s, core])):
                on.wait_recv()

                @pl.when(more[h])
                def _():
                    on.start()

                share.start()

        for h, (on, share) in enumerate(copies(colb.at[s, core])):
            waits.append((more[h], on))
            waits.append((None, share))

    def chain_done(s, owner, delta):
        for h in range(2):
            block = colb.at[s, 1 - core, owner, h]
            k = (s, delta, h)
            remote(block, block, p_ss.at[k], p_rs.at[k], partner).wait_recv()

    counts = []
    for p in range(n):
        count = jnp.float32(0)
        for k in range(NADJ):
            count = count + jnp.where(adj[0, k] % n == p, 1.0, 0.0).astype(F32)
        counts.append(count)

    loads[0].wait()
    for s in range(ITERS):
        base = exc if s == 0 else sol_ref
        rounded = base[...].astype(BF16)
        grp[s, c] = rounded.reshape(2, hs, ne)

        for t in range(1, half_n + 1):
            for i in range(2):
                for d in range(2):
                    h = halves(d, t)
                    if i < len(h):
                        copy = ring(grp, g_ss, g_rs, s, d, t, h[i])
                        if t > 1:
                            ring(grp, g_ss, g_rs, s, d, t - 1, h[i], True).wait_recv()
                        copy.start()
                        waits.append((None, copy))
            if t > 1:
                for d in range(2):
                    for h in halves(d, t - 1):
                        if h not in halves(d, t):
                            ring(grp, g_ss, g_rs, s, d, t - 1, h, True).wait_recv()
            if t == 1:
                chain_order = [(c, 0)]
        for d in range(2):
            for h in halves(d, half_n):
                ring(grp, g_ss, g_rs, s, d, half_n, h, True).wait_recv()
        chain_order = [((c + k) % n, k) for k in range(n)]

        @pl.when(pos == 0)
        def _():
            colb[s, core] = grp[s]

        if s == 0:
            loads[1].wait()
        group = grp[s].reshape(rb, ne)
        for h in range(2):
            rows = pl.ds(h * (m // 2), m // 2)
            value = jnp.dot(interp[rows, :], group, preferred_element_type=F32)
            trc[s, c, h] = value.astype(BF16)
            for d in range(2):
                copy = ring(trc, t_ss, t_rs, s, d, 1, h)
                copy.start()
                waits.append((None, copy))

        def trace_step(t):
            for i in range(2):
                for d in range(2):
                    h = halves(d, t)
                    if i < len(h):
                        ring(trc, t_ss, t_rs, s, d, t - 1, h[i], True).wait_recv()
                        copy = ring(trc, t_ss, t_rs, s, d, t, h[i])
                        copy.start()
                        waits.append((None, copy))
            for d in range(2):
                for h in halves(d, t - 1):
                    if h not in halves(d, t):
                        ring(trc, t_ss, t_rs, s, d, t - 1, h, True).wait_recv()

        for k, (owner, delta) in enumerate(chain_order):
            chain(s, owner, delta)
            if k >= 1 and k + 1 <= half_n:
                trace_step(k + 1)
        for owner, delta in chain_order:
            chain_done(s, owner, delta)

        column = colb[s].reshape(2 * rb, ne)
        for i in range(tiles):
            if s == 0:
                loads[2 + i].wait()
            rows = pl.ds(i * tile, tile)
            acc[rows, :] = jnp.dot(surf[rows, :], column, preferred_element_type=F32)

        if s == 0:
            loads[-1].wait()
        own = trc[s, c].reshape(m, ne)
        combined = jnp.dot(dtn[...], own, preferred_element_type=F32)
        combined = combined + (1.0 + face_weight * NADJ) * own.astype(F32)
        for d in range(2):
            for h in halves(d, half_n):
                ring(trc, t_ss, t_rs, s, d, half_n, h, True).wait_recv()
        neighbours = counts[0] * trc[s, 0].reshape(m, ne).astype(F32)
        for p in range(1, n):
            neighbours = neighbours + counts[p] * trc[s, p].reshape(m, ne).astype(F32)
        response = combined - face_weight * neighbours
        turned = response.T.astype(BF16)
        volume = jnp.dot(turned, interp[...], preferred_element_type=F32)
        part[...] = (acc[...] + volume.T).reshape(n, 2, hs, ne)

        def summing(d, t, h):
            k = (s, d, t - 1, h)
            return remote(sbuf.at[k], rbuf.at[k], r_ss.at[k], r_rs.at[k], right if d == 0 else left)

        for t in range(half_n, 0, -1):
            for i in range(2):
                for d in range(2):
                    hh = halves(d, t)
                    if i < len(hh):
                        h = hh[i]
                        target = (c + t) % n if d == 0 else (c + n - t) % n
                        value = part[target, h]
                        if t < half_n and h in halves(d, t + 1):
                            summing(d, t + 1, h).wait_recv()
                            value = value + rbuf[s, d, t, h].astype(F32)
                        sbuf[s, d, t - 1, h] = value.astype(BF16)
                        copy = summing(d, t, h)
                        copy.start()
                        waits.append((None, copy))
        for h in range(2):
            rows = pl.ds(h * hs, hs)
            total = part[c, h]
            for d in range(2):
                summing(d, 1, h).wait_recv()
                total = total + rbuf[s, d, 0, h].astype(F32)
            current = base[rows, :]
            residual = exc[rows, :] - current - total
            res_ref[rows, :] = residual
            sol_ref[rows, :] = current + damping * residual

    for condition, copy in waits:
        if condition is None:
            copy.wait_send()
        else:
            pl.when(condition)(copy.wait_send)


def local(surface, excitation, dtn_blocks, interp_blocks, adjacency):
    R, n = lax.axis_size("row"), lax.axis_size("col")
    shard, ne = excitation.shape
    m, rb = interp_blocks.shape[1:]
    hs = shard // 2
    tile = min(512, surface.shape[0])
    assert R == 2 * n and n % 2 == 0 and n & (n - 1) == 0
    hops = n // 2
    vmem, hbm = pltpu.VMEM, pl.BlockSpec(memory_space=pl.ANY)
    dma = pltpu.SemaphoreType.DMA
    out = jax.ShapeDtypeStruct((shard, ne), F32)
    S = ITERS
    ring_sems = [dma((S, 2, hops, 2))] * 2
    chain_sems = [dma((S, n, 2))] * 2
    return pl.pallas_call(
        functools.partial(kernel, R, n, tile),
        out_shape=(out, out),
        in_specs=[hbm, hbm, hbm, hbm, pl.BlockSpec(memory_space=pltpu.SMEM)],
        out_specs=(pl.BlockSpec(memory_space=vmem),) * 2,
        scratch_shapes=[
            vmem((shard, ne), F32),
            vmem((m, rb), BF16),
            vmem(surface.shape, BF16),
            vmem((m, m), BF16),
            vmem((S, n, 2, hs, ne), BF16),
            vmem((S, 2, n, 2, hs, ne), BF16),
            vmem((S, n, 2, m // 2, ne), BF16),
            vmem((rb, ne), F32),
            vmem((n, 2, hs, ne), F32),
            vmem((S, 2, hops, 2, hs, ne), BF16),
            vmem((S, 2, hops, 2, hs, ne), BF16),
            dma((3 + surface.shape[0] // tile,)),
            *ring_sems, *ring_sems, *chain_sems, *chain_sems, *ring_sems,
        ],
        compiler_params=pltpu.CompilerParams(
            collective_id=0, has_side_effects=True, vmem_limit_bytes=60 * 2**20
        ),
    )(excitation, interp_blocks.reshape(m, rb), surface, dtn_blocks.reshape(m, m), adjacency)


def solution(mesh):
    in_specs = (
        P("row", "col"),
        P(("row", "col"), None),
        P(("row", "col"), None, None),
        P(("row", "col"), None, None),
        P(("row", "col"), None),
    )
    out_specs = (P(("row", "col"), None), P(("row", "col"), None))
    return jax.shard_map(local, mesh=mesh, in_specs=in_specs, out_specs=out_specs, check_vma=False)
```

```python
import functools

import jax
import jax.numpy as jnp
from jax import lax
from jax.experimental import pallas as pl
from jax.experimental.pallas import tpu as pltpu
from jax.sharding import PartitionSpec as P

ITERS = 2
NADJ = 6

damping = 0.25
face_weight = 0.25
F32, BF16 = jnp.float32, jnp.bfloat16


def xor(a, b, bits):
    total = 0
    for i in range(bits):
        x, y = a // 2**i % 2, b // 2**i % 2
        total = total + (x + y - 2 * x * y) * 2**i
    return total


def gray(p, bits):
    return xor(p, p // 2, bits)


def ungray(g, bits):
    total, above = 0, 0
    for i in reversed(range(bits)):
        bit = g // 2**i % 2
        above = above + bit - 2 * above * bit
        total = total + above * 2**i
    return total


def kernel(
    R, n, tile,
    exc_hbm, interp_hbm, surf_hbm, dtn_hbm, adj,
    sol_ref, res_ref,
    exc, interp, surf, dtn, grp, colb, trc, acc, part, sbuf, rbuf,
    load_sem, g_ss, g_rs, t_ss, t_rs, c_ss, c_rs, p_ss, p_rs, r_ss, r_rs,
):
    half_n = n // 2
    bits = n.bit_length() - 1
    _, _, hs, ne = grp.shape[1:]
    m = interp.shape[0]
    rb = interp.shape[1]
    tiles = surf.shape[0] // tile
    r, c = lax.axis_index("row"), lax.axis_index("col")
    core, chip = r % 2, r // 2
    pos = ungray(xor(chip, c, bits), bits)
    right, left = (r, (c + 1) % n), (r, (c + n - 1) % n)
    partner = (chip * 2 + 1 - core, c)
    gnext = (xor(gray((pos + 1) % n, bits), c, bits) * 2 + core, c)
    gprev = (xor(gray((pos + n - 1) % n, bits), c, bits) * 2 + core, c)

    loads = [
        pltpu.make_async_copy(exc_hbm, exc, load_sem.at[0]),
        pltpu.make_async_copy(interp_hbm, interp, load_sem.at[1]),
    ]
    for i in range(tiles):
        rows = pl.ds(i * tile, tile)
        loads.append(pltpu.make_async_copy(surf_hbm.at[rows], surf.at[rows], load_sem.at[3 + i]))
    loads.append(pltpu.make_async_copy(dtn_hbm, dtn, load_sem.at[2]))
    for load in loads:
        load.start()

    barrier = pltpu.get_barrier_semaphore()
    for device in (left, right, partner, gnext, gprev):
        pl.semaphore_signal(barrier, inc=1, device_id=device, device_id_type=pl.DeviceIdType.MESH)
    pl.semaphore_wait(barrier, 5)

    def remote(src, dst, ss, rs, device):
        return pltpu.make_async_remote_copy(
            src_ref=src, dst_ref=dst, send_sem=ss, recv_sem=rs,
            device_id=device, device_id_type=pl.DeviceIdType.MESH,
        )

    def ring(buf, ss, rs, s, d, t, h, receive=False):
        hop = t if receive else t - 1
        owner = (c + n - hop) % n if d == 0 else (c + hop) % n
        block = buf.at[s, owner, h]
        return remote(block, block, ss.at[s, d, t - 1, h], rs.at[s, d, t - 1, h], right if d == 0 else left)

    def halves(d, t):
        if t == half_n:
            return (d,)
        return (d, 1 - d)

    waits = []

    def chain_copies(src, s, owner, delta, h):
        block = src.at[owner, h]
        dst = colb.at[s, core, owner, h]
        k = (s, delta, h)
        return (
            remote(block, dst, c_ss.at[k], c_rs.at[k], gnext if h == 0 else gprev),
            remote(block, dst, p_ss.at[k], p_rs.at[k], partner),
        )

    def chain_source(s, deltas):
        @pl.when(pos == 0)
        def _():
            for delta in deltas:
                for h in range(2):
                    on, _ = chain_copies(grp.at[s], s, (c + delta) % n, delta, h)
                    on.start()
            for delta in deltas:
                for h in range(2):
                    _, share = chain_copies(grp.at[s], s, (c + delta) % n, delta, h)
                    share.start()

    arrival = [0] + sorted(range(1, n), key=lambda k: min(k, n - k))

    def chain_relay(s, phase):
        for q in range(1, n):
            pieces = []
            for k, delta in enumerate(arrival):
                for h in range(2):
                    hops = q if h == 0 else n - q
                    own_phase = 2 if hops > 1 else (0 if k == 0 else 1)
                    if own_phase == phase:
                        pieces.append((k + hops, -hops, k, delta, h))
            pieces.sort()

            @pl.when(pos == q)
            def _():
                for _, _, _, delta, h in pieces:
                    on, share = chain_copies(colb.at[s, core], s, (c + delta) % n, delta, h)
                    on.wait_recv()
                    if q != (n - 1 if h == 0 else 1):
                        on.start()
                    share.start()

    def chain_sent(s):
        for delta in range(n):
            for h in range(2):
                on, share = chain_copies(colb.at[s, core], s, (c + delta) % n, delta, h)
                waits.append((pos != (n - 1 if h == 0 else 1), on))
                waits.append((None, share))

    def chain_done(s, owner, delta):
        for h in range(2):
            block = colb.at[s, 1 - core, owner, h]
            k = (s, delta, h)
            remote(block, block, p_ss.at[k], p_rs.at[k], partner).wait_recv()

    counts = []
    for p in range(n):
        count = jnp.float32(0)
        for k in range(NADJ):
            count = count + jnp.where(adj[0, k] % n == p, 1.0, 0.0).astype(F32)
        counts.append(count)

    def send_own(s, h, value):
        grp[s, c, h] = value.astype(BF16)
        for d in range(2):
            copy = ring(grp, g_ss, g_rs, s, d, 1, h)
            copy.start()
            waits.append((None, copy))

    loads[0].wait()
    for s in range(ITERS):
        base = exc if s == 0 else sol_ref
        if s == 0:
            for h in range(2):
                send_own(0, h, exc[pl.ds(h * hs, hs), :])
        chain_source(s, arrival[:1])

        for t in range(2, half_n + 1):
            for i in range(2):
                for d in range(2):
                    h = halves(d, t)
                    if i < len(h):
                        copy = ring(grp, g_ss, g_rs, s, d, t, h[i])
                        ring(grp, g_ss, g_rs, s, d, t - 1, h[i], True).wait_recv()
                        copy.start()
                        waits.append((None, copy))
            if t > 1:
                for d in range(2):
                    for h in halves(d, t - 1):
                        if h not in halves(d, t):
                            ring(grp, g_ss, g_rs, s, d, t - 1, h, True).wait_recv()
        for d in range(2):
            for h in halves(d, half_n):
                ring(grp, g_ss, g_rs, s, d, half_n, h, True).wait_recv()
        chain_source(s, arrival[1:])
        chain_relay(s, 0)

        @pl.when(pos == 0)
        def _():
            colb[s, core] = grp[s]

        if s == 0:
            loads[1].wait()
        group = grp[s].reshape(rb, ne)
        for h in range(2):
            rows = pl.ds(h * (m // 2), m // 2)
            value = jnp.dot(interp[rows, :], group, preferred_element_type=F32)
            trc[s, c, h] = value.astype(BF16)
            for d in range(2):
                copy = ring(trc, t_ss, t_rs, s, d, 1, h)
                copy.start()
                waits.append((None, copy))

        def trace_step(t):
            for i in range(2):
                for d in range(2):
                    h = halves(d, t)
                    if i < len(h):
                        ring(trc, t_ss, t_rs, s, d, t - 1, h[i], True).wait_recv()
                        copy = ring(trc, t_ss, t_rs, s, d, t, h[i])
                        copy.start()
                        waits.append((None, copy))
            for d in range(2):
                for h in halves(d, t - 1):
                    if h not in halves(d, t):
                        ring(trc, t_ss, t_rs, s, d, t - 1, h, True).wait_recv()

        chain_relay(s, 1)
        for t in range(2, half_n + 1):
            trace_step(t)
        chain_relay(s, 2)
        for delta in range(n):
            chain_done(s, (c + delta) % n, delta)
        chain_sent(s)

        column = colb[s].reshape(2 * rb, ne)
        for i in range(tiles):
            if s == 0:
                loads[2 + i].wait()
            rows = pl.ds(i * tile, tile)
            acc[rows, :] = jnp.dot(surf[rows, :], column, preferred_element_type=F32)

        if s == 0:
            loads[-1].wait()
        own = trc[s, c].reshape(m, ne)
        combined = jnp.dot(dtn[...], own, preferred_element_type=F32)
        combined = combined + (1.0 + face_weight * NADJ) * own.astype(F32)
        for d in range(2):
            for h in halves(d, half_n):
                ring(trc, t_ss, t_rs, s, d, half_n, h, True).wait_recv()
        neighbours = counts[0] * trc[s, 0].reshape(m, ne).astype(F32)
        for p in range(1, n):
            neighbours = neighbours + counts[p] * trc[s, p].reshape(m, ne).astype(F32)
        response = combined - face_weight * neighbours
        turned = response.T.astype(BF16)
        volume = jnp.dot(turned, interp[...], preferred_element_type=F32)
        part[...] = (acc[...] + volume.T).reshape(n, 2, hs, ne)

        def summing(d, t, h):
            k = (s, d, t - 1, h)
            return remote(sbuf.at[k], rbuf.at[k], r_ss.at[k], r_rs.at[k], right if d == 0 else left)

        for t in range(half_n, 0, -1):
            for i in range(2):
                for d in range(2):
                    hh = halves(d, t)[:: -1 if t == half_n - 1 else 1]
                    if i < len(hh):
                        h = hh[i]
                        target = (c + t) % n if d == 0 else (c + n - t) % n
                        value = part[target, h]
                        if t < half_n and h in halves(d, t + 1):
                            summing(d, t + 1, h).wait_recv()
                            value = value + rbuf[s, d, t, h].astype(F32)
                        sbuf[s, d, t - 1, h] = value.astype(BF16)
                        copy = summing(d, t, h)
                        copy.start()
                        waits.append((None, copy))
        for h in range(2):
            rows = pl.ds(h * hs, hs)
            total = part[c, h]
            for d in range(2):
                summing(d, 1, h).wait_recv()
                total = total + rbuf[s, d, 0, h].astype(F32)
            current = base[rows, :]
            residual = exc[rows, :] - current - total
            updated = current + damping * residual
            if s + 1 < ITERS:
                send_own(s + 1, h, updated)
            res_ref[rows, :] = residual
            sol_ref[rows, :] = updated

    for condition, copy in waits:
        if condition is None:
            copy.wait_send()
        else:
            pl.when(condition)(copy.wait_send)


def local(surface, excitation, dtn_blocks, interp_blocks, adjacency):
    R, n = lax.axis_size("row"), lax.axis_size("col")
    shard, ne = excitation.shape
    m, rb = interp_blocks.shape[1:]
    hs = shard // 2
    tile = min(512, surface.shape[0])
    assert R == 2 * n and n % 2 == 0 and n & (n - 1) == 0
    hops = n // 2
    vmem, hbm = pltpu.VMEM, pl.BlockSpec(memory_space=pl.ANY)
    dma = pltpu.SemaphoreType.DMA
    out = jax.ShapeDtypeStruct((shard, ne), F32)
    S = ITERS
    ring_sems = [dma((S, 2, hops, 2))] * 2
    chain_sems = [dma((S, n, 2))] * 2
    return pl.pallas_call(
        functools.partial(kernel, R, n, tile),
        out_shape=(out, out),
        in_specs=[hbm, hbm, hbm, hbm, pl.BlockSpec(memory_space=pltpu.SMEM)],
        out_specs=(pl.BlockSpec(memory_space=vmem),) * 2,
        scratch_shapes=[
            vmem((shard, ne), F32),
            vmem((m, rb), BF16),
            vmem(surface.shape, BF16),
            vmem((m, m), BF16),
            vmem((S, n, 2, hs, ne), BF16),
            vmem((S, 2, n, 2, hs, ne), BF16),
            vmem((S, n, 2, m // 2, ne), BF16),
            vmem((rb, ne), F32),
            vmem((n, 2, hs, ne), F32),
            vmem((S, 2, hops, 2, hs, ne), BF16),
            vmem((S, 2, hops, 2, hs, ne), BF16),
            dma((3 + surface.shape[0] // tile,)),
            *ring_sems, *ring_sems, *chain_sems, *chain_sems, *ring_sems,
        ],
        compiler_params=pltpu.CompilerParams(
            collective_id=0, has_side_effects=True, vmem_limit_bytes=60 * 2**20
        ),
    )(excitation, interp_blocks.reshape(m, rb), surface, dtn_blocks.reshape(m, m), adjacency)


def solution(mesh):
    in_specs = (
        P("row", "col"),
        P(("row", "col"), None),
        P(("row", "col"), None, None),
        P(("row", "col"), None, None),
        P(("row", "col"), None),
    )
    out_specs = (P(("row", "col"), None), P(("row", "col"), None))
    return jax.shard_map(local, mesh=mesh, in_specs=in_specs, out_specs=out_specs, check_vma=False)
```
